32 devices in a mesh: dp: 2 (over x), tp: 4 (over z), section: 4 (over y, core).
Axes of the slice: x: 2, y: 2, z: 4, core: 2. Of those that a mesh axis runs over, the one named last changes fastest.
Arguments:
- tokens: bfloat16 [256, 2304], P('dp', 'section'), may hold values from -6 to 6
- hidden_grad: bfloat16 [256, 18432], P('dp', ('tp', 'section')), may hold values from -6 to 6
- norm_gain: float32 [2304], replicated, may hold values from 0.5 to 1.5
- w_gate: bfloat16 [2304, 18432], P('dp', ('tp', 'section')), may hold values from -0.125 to 0.125
- w_up: bfloat16 [2304, 18432], P('dp', ('tp', 'section')), may hold values from -0.125 to 0.125
Outputs:
- grad_tokens: bfloat16 [256, 2304], P('dp', ('tp', 'section'))
- grad_gain: float32 [2304], P(('tp', 'section'))
- grad_gate: bfloat16 [2304, 18432], P('dp', ('tp', 'section'))
- grad_up: bfloat16 [2304, 18432], P('dp', ('tp', 'section'))
The draws below stay inside these ranges and needn't reach their ends.
All inputs are finite; a program needn't handle non-finite values.
Results may differ from the reference program's by a relative error of at most 0.018.
Values may be sent and summed in bfloat16 or wider, within the bound.
A program may use at most 128 MiB of HBM per device.

```python
import jax
import jax.numpy as jnp
from jax import lax

D = 2304
FF = 18432
TOK_DEV = 128
TOKENS = 256
N_DP = 2
N_TP = 4
N_SECTION = 4


def level_of(own_key, extent, cuts, smallest, top_value):
    gain, own = 1.0, jax.random.fold_in(own_key, 6)
    for position, shards_of in cuts:
        heights = jnp.exp(jax.random.uniform(jax.random.fold_in(own, position), (shards_of,), jnp.float32, smallest / len(cuts), top_value / len(cuts)))
        gain = gain * jnp.repeat(heights, extent[position] // shards_of).reshape([-1 if axis == position else 1 for axis in range(len(extent))])
    return gain


def centred(key, dims, deviation, bound, cuts=(), held_as=jnp.bfloat16):
    drawn = jax.random.normal(key, dims, jnp.float32) * deviation
    if len(cuts) > 0:
        drawn = level_of(key, dims, cuts, -0.22, 0.18) * drawn
    return jnp.clip(drawn, min=-bound, max=bound).astype(held_as)


def setup_inputs(seed: int = 0) -> dict:
    key_list = jax.random.split(jax.random.key(seed), 6)
    return {
        "tokens": centred(key_list[0], (TOKENS, D), 1.0, 6.0, ((0, 2), (1, 4))),
        "hidden_grad": centred(key_list[1], (TOKENS, FF), 1.0, 6.0, ((0, 2), (1, 16))),
        "norm_gain": jnp.clip(1.0 + 0.1 * jax.random.normal(key_list[2], (D,), jnp.float32), 0.5, 1.5),
        "w_gate": centred(key_list[3], (D, FF), D ** -0.5, 0.125, ((0, 2), (1, 16))),
        "w_up": centred(key_list[4], (D, FF), D ** -0.5, 0.125, ((0, 2), (1, 16))),
    }


epsilon = 1e-06

def gated_unit(gate, up):
    return jax.nn.gelu(gate, approximate=True) * up

def rounded(value):
    return lax.optimization_barrier(value.astype(jnp.bfloat16)).astype(jnp.float32)

def reference(tokens, hidden_grad, norm_gain, w_gate, w_up):
    groups = N_TP * N_SECTION
    fwidth = FF // groups
    gate_blocks = w_gate.astype(jnp.float32).reshape(D, groups, fwidth)
    up_blocks = w_up.astype(jnp.float32).reshape(D, groups, fwidth)

    def one_group(index, carry):
        sum_gate, sum_up, gain_total, result = carry
        start = (index * TOK_DEV).astype(jnp.int32)
        rows_in = lax.dynamic_slice_in_dim(tokens, start, TOK_DEV, 0)
        back = lax.dynamic_slice_in_dim(hidden_grad, start, TOK_DEV, 0).astype(jnp.float32)
        inputs = rows_in.astype(jnp.float32)
        inv_rms = lax.rsqrt(lax.optimization_barrier(jnp.mean(inputs * inputs, axis=1)) + epsilon)
        normed = (inputs * inv_rms[:, None] * norm_gain).astype(jnp.bfloat16)
        gate = jnp.dot(normed, w_gate, preferred_element_type=jnp.float32)
        up = jnp.dot(normed, w_up, preferred_element_type=jnp.float32)
        hidden, pull = jax.vjp(gated_unit, gate, up)
        d_gate, d_up = pull(back)
        d_gate = d_gate.astype(jnp.bfloat16)
        d_up = d_up.astype(jnp.bfloat16)
        gate_split = d_gate.astype(jnp.float32).reshape(TOK_DEV, groups, fwidth)
        up_split = d_up.astype(jnp.float32).reshape(TOK_DEV, groups, fwidth)
        parts = jnp.einsum('rbf,dbf->bdr', gate_split, gate_blocks) + jnp.einsum('rbf,dbf->bdr', up_split, up_blocks)
        d_normed = lax.optimization_barrier(jnp.sum(rounded(parts), axis=0)).T
        gain_total = gain_total + lax.optimization_barrier(jnp.sum(d_normed * inputs * inv_rms[:, None], axis=0))
        row_sum = lax.optimization_barrier(jnp.sum(inputs * norm_gain * d_normed, axis=1))
        grad_rows = inv_rms[:, None] * norm_gain * d_normed - inputs * (inv_rms ** 3 * row_sum / D)[:, None]
        result = lax.dynamic_update_slice(result, grad_rows.astype(jnp.bfloat16), (start, jnp.zeros((), jnp.int32)))
        sum_gate = sum_gate + rounded(jnp.dot(normed.T, d_gate, preferred_element_type=jnp.float32))
        sum_up = sum_up + rounded(jnp.dot(normed.T, d_up, preferred_element_type=jnp.float32))
        return (sum_gate, sum_up, gain_total, result)
    empty = jnp.zeros((D, FF), jnp.float32)
    start_carry = (empty, empty, jnp.zeros((D,), jnp.float32), jnp.zeros((TOKENS, D), jnp.bfloat16))
    sum_gate, sum_up, gain_total, result = lax.fori_loop(0, N_DP, one_group, start_carry)
    return (result, gain_total, sum_gate.astype(jnp.bfloat16), sum_up.astype(jnp.bfloat16))
```

```python
import jax
import jax.numpy as jnp
from jax import lax
from jax.sharding import PartitionSpec as P

D = 2304


epsilon = 1e-06


def gated_unit(gate, up):
    return jax.nn.gelu(gate, approximate=True) * up


def shards(tokens, hidden_grad, norm_gain, w_gate, w_up):
    n_dp = lax.axis_size("dp")
    n_model = lax.axis_size(("tp", "section"))
    rows_in = lax.all_gather(tokens, "section", axis=1, tiled=True)
    inputs = rows_in.astype(jnp.float32)
    inv_rms = lax.rsqrt(jnp.mean(inputs * inputs, axis=1) + epsilon)
    normed = (inputs * inv_rms[:, None] * norm_gain).astype(jnp.bfloat16)
    per_device, features = normed.shape
    cols_normed = lax.all_to_all(normed, "dp", split_axis=1, concat_axis=0, tiled=True)
    width = w_gate.shape[1]
    part_gate = jnp.dot(cols_normed, w_gate, preferred_element_type=jnp.float32)
    part_up = jnp.dot(cols_normed, w_up, preferred_element_type=jnp.float32)
    parts = jnp.concatenate([part_gate, part_up], axis=1).astype(jnp.bfloat16)
    parts = lax.all_to_all(parts, "dp", split_axis=0, concat_axis=0, tiled=True)
    sums = jnp.sum(parts.reshape(n_dp, per_device, 2 * width).astype(jnp.float32), axis=0)
    gate, up = sums[:, :width], sums[:, width:]
    hidden, pull = jax.vjp(gated_unit, gate, up)
    d_both = jnp.concatenate(pull(hidden_grad.astype(jnp.float32)), axis=1).astype(jnp.bfloat16)
    d_all = lax.all_gather(d_both, "dp", axis=0, tiled=True)
    d_gate, d_up = d_all[:, :width], d_all[:, width:]
    contract_cols = (((1,), (1,)), ((), ()))
    contract_rows = (((0,), (0,)), ((), ()))
    first = lax.dot_general(w_gate, d_gate, contract_cols, preferred_element_type=jnp.float32)
    second = lax.dot_general(w_up, d_up, contract_cols, preferred_element_type=jnp.float32)
    own_width = features // n_model
    per_row = n_model // n_dp
    d_part = (first + second).astype(jnp.bfloat16)
    d_part = d_part.reshape(per_row, own_width, n_dp, per_device).transpose(2, 0, 1, 3)
    d_part = d_part.reshape(n_model * own_width, per_device)
    d_columns = lax.psum_scatter(d_part, ("tp", "section"), scatter_dimension=0, tiled=True)
    moves = [
        (i * n_model + o * per_row + r, o * n_model + i * per_row + r)
        for i in range(n_dp)
        for o in range(n_dp)
        for r in range(per_row)
    ]
    d_columns = lax.ppermute(d_columns, ("dp", "tp", "section"), moves)
    d_normed = d_columns.astype(jnp.float32).T
    offset = lax.axis_index(("tp", "section")) * own_width
    own_inputs = lax.dynamic_slice_in_dim(inputs, offset, own_width, 1)
    own_gain = lax.dynamic_slice_in_dim(norm_gain, offset, own_width, 0)
    gain_part = jnp.sum(d_normed * own_inputs * inv_rms[:, None], axis=0)
    row_part = jnp.sum(own_inputs * own_gain * d_normed, axis=1)
    grad_gain = lax.psum(gain_part, "dp")
    row_sum = lax.psum(row_part, ("tp", "section"))
    grad_tokens = (
        inv_rms[:, None] * own_gain * d_normed
        - own_inputs * (inv_rms**3 * row_sum / features)[:, None]
    )
    grad_gate = lax.dot_general(cols_normed, d_gate, contract_rows, preferred_element_type=jnp.float32)
    grad_up = lax.dot_general(cols_normed, d_up, contract_rows, preferred_element_type=jnp.float32)
    return (
        grad_tokens.astype(jnp.bfloat16),
        grad_gain,
        grad_gate.astype(jnp.bfloat16),
        grad_up.astype(jnp.bfloat16),
    )


def solution(mesh):
    in_specs = (
        P("dp", "section"),
        P("dp", ("tp", "section")),
        P(),
        P("dp", ("tp", "section")),
        P("dp", ("tp", "section")),
    )
    out_specs = (
        P("dp", ("tp", "section")),
        P(("tp", "section")),
        P("dp", ("tp", "section")),
        P("dp", ("tp", "section")),
    )
    return jax.shard_map(shards, mesh=mesh, in_specs=in_specs, out_specs=out_specs, check_vma=False)
```

```python
import functools

import jax
import jax.numpy as jnp
from jax import lax
from jax.experimental import pallas as pl
from jax.experimental.pallas import tpu as pltpu
from jax.sharding import PartitionSpec as P

D = 2304


epsilon = 1e-06


def gated_unit(gate, up):
    return jax.nn.gelu(gate, approximate=True) * up


def shards(tokens, hidden_grad, norm_gain, w_gate, w_up):
    n_dp = lax.axis_size("dp")
    n_model = lax.axis_size(("tp", "section"))
    rows_in = lax.all_gather(tokens, "section", axis=1, tiled=True)
    inputs = rows_in.astype(jnp.float32)
    inv_rms = lax.rsqrt(jnp.mean(inputs * inputs, axis=1) + epsilon)
    normed = (inputs * inv_rms[:, None] * norm_gain).astype(jnp.bfloat16)
    per_device, features = normed.shape
    cols_normed = lax.all_to_all(normed, "dp", split_axis=1, concat_axis=0, tiled=True)
    width = w_gate.shape[1]
    part_gate = jnp.dot(cols_normed, w_gate, preferred_element_type=jnp.float32)
    part_up = jnp.dot(cols_normed, w_up, preferred_element_type=jnp.float32)
    parts = jnp.concatenate([part_gate, part_up], axis=1).astype(jnp.bfloat16)
    parts = lax.all_to_all(parts, "dp", split_axis=0, concat_axis=0, tiled=True)
    sums = jnp.sum(parts.reshape(n_dp, per_device, 2 * width).astype(jnp.float32), axis=0)
    gate, up = sums[:, :width], sums[:, width:]
    hidden, pull = jax.vjp(gated_unit, gate, up)
    d_both = jnp.concatenate(pull(hidden_grad.astype(jnp.float32)), axis=1).astype(jnp.bfloat16)
    d_all = lax.all_gather(d_both, "dp", axis=0, tiled=True)
    d_gate, d_up = d_all[:, :width], d_all[:, width:]
    contract_cols = (((1,), (1,)), ((), ()))
    contract_rows = (((0,), (0,)), ((), ()))
    first = lax.dot_general(w_gate, d_gate, contract_cols, preferred_element_type=jnp.float32)
    second = lax.dot_general(w_up, d_up, contract_cols, preferred_element_type=jnp.float32)
    own_width = features // n_model
    per_row = n_model // n_dp
    d_part = (first + second).astype(jnp.bfloat16)
    d_part = d_part.reshape(per_row, own_width, n_dp, per_device).transpose(2, 0, 1, 3)
    d_part = d_part.reshape(n_model * own_width, per_device)
    d_columns = lax.psum_scatter(d_part, ("tp", "section"), scatter_dimension=0, tiled=True)
    moves = [
        (i * n_model + o * per_row + r, o * n_model + i * per_row + r)
        for i in range(n_dp)
        for o in range(n_dp)
        for r in range(per_row)
    ]
    d_columns = lax.ppermute(d_columns, ("dp", "tp", "section"), moves)
    d_normed = d_columns.astype(jnp.float32).T
    offset = lax.axis_index(("tp", "section")) * own_width
    own_inputs = lax.dynamic_slice_in_dim(inputs, offset, own_width, 1)
    own_gain = lax.dynamic_slice_in_dim(norm_gain, offset, own_width, 0)
    gain_part = jnp.sum(d_normed * own_inputs * inv_rms[:, None], axis=0)
    row_part = jnp.sum(own_inputs * own_gain * d_normed, axis=1)
    grad_gain = lax.psum(gain_part, "dp")
    row_sum = lax.psum(row_part, ("tp", "section"))
    grad_tokens = (
        inv_rms[:, None] * own_gain * d_normed
        - own_inputs * (inv_rms**3 * row_sum / features)[:, None]
    )
    grad_gate = lax.dot_general(cols_normed, d_gate, contract_rows, preferred_element_type=jnp.float32)
    grad_up = lax.dot_general(cols_normed, d_up, contract_rows, preferred_element_type=jnp.float32)
    return (
        grad_tokens.astype(jnp.bfloat16),
        grad_gain,
        grad_gate.astype(jnp.bfloat16),
        grad_up.astype(jnp.bfloat16),
    )


MESH = pl.DeviceIdType.MESH
SQRT_2_OVER_PI = 0.7978845608028654
CUBIC = 0.044715
CHUNKS = 3
CONTRACT_COLS = (((1,), (1,)), ((), ()))


def exchange_kernel(
    full,
    x_t,
    gain_sec,
    gain_own,
    back_hbm,
    wg_hbm,
    wu_hbm,
    grad_t,
    prod_out,
    xg_out,
    d_out,
    wg,
    wu,
    back,
    xg_send,
    xg,
    xn,
    slab,
    squares,
    part_send,
    part_recv,
    own_part,
    d_all,
    pieces,
    incoming,
    moved,
    move_send,
    rows,
    prods,
    load_sem,
    tok_send,
    tok_recv,
    slab_send,
    slab_recv,
    sq_send,
    sq_recv,
    part_ssem,
    part_rsem,
    d_ssem,
    d_rsem,
    piece_ssem,
    piece_rsem,
    last_send,
    last_recv,
    row_ssem,
    row_rsem,
):
    i, t, s = lax.axis_index("dp"), lax.axis_index("tp"), lax.axis_index("section")
    other = 1 - i
    sec_rows, per_device = x_t.shape
    own = slab.shape[0]
    half, q = s // 2, lax.rem(s, 2)
    sibling, across = s + 1 - 2 * q, s + 2 - 4 * half
    ck = wg.shape[2]
    width = CHUNKS * ck

    def to(d, tt, ss):
        return {"dp": d, "tp": tt, "section": ss}

    def send(src, dst, ssem, rsem, target):
        return pltpu.make_async_remote_copy(
            src_ref=src, dst_ref=dst, send_sem=ssem, recv_sem=rsem, device_id=target, device_id_type=MESH
        )

    barrier = pltpu.get_barrier_semaphore()
    group = [(dt, ds) for dt in range(4) for ds in range(4) if dt + ds > 0]
    swap_tp = t + 2 - 4 * (t // 2)
    everyone = [to(i, lax.rem(t + dt, 4), lax.rem(s + ds, 4)) for dt, ds in group]
    everyone += [to(other, t, s), to(other, swap_tp, s)]
    for target in everyone:
        pl.semaphore_signal(barrier, inc=1, device_id=target, device_id_type=MESH)

    loads = []
    for k in range(CHUNKS):
        cols = pl.ds(k * ck, ck)
        loads.append(
            (
                pltpu.make_async_copy(wg_hbm.at[:, cols], wg.at[k], load_sem.at[0, k]),
                pltpu.make_async_copy(wu_hbm.at[:, cols], wu.at[k], load_sem.at[1, k]),
                pltpu.make_async_copy(back_hbm.at[:, cols], back.at[k], load_sem.at[2, k]),
            )
        )
        for load in loads[-1]:
            load.start()

    raw = x_t[...].astype(jnp.float32)
    scaled = (raw * gain_sec[...]).astype(jnp.bfloat16)
    xg_send[...] = scaled
    squares[0] = jnp.broadcast_to(jnp.sum(raw * raw, axis=0, keepdims=True), squares.shape[1:])
    my_rows = pl.ds(pl.multiple_of(q * sec_rows, 16), sec_rows)

    pl.semaphore_wait(barrier, len(everyone))

    over_dp = send(xg_send, xg.at[i, my_rows], tok_send.at[0], tok_recv.at[0], to(other, t, s))
    over_y = [
        send(xg_send, xg.at[i, my_rows], tok_send.at[1], tok_recv.at[1], to(i, t, across)),
        send(xg.at[other, my_rows], xg.at[other, my_rows], tok_send.at[2], tok_recv.at[2], to(i, t, across)),
    ]
    over_core = [
        send(xg.at[g, my_rows], xg.at[g, my_rows], tok_send.at[3 + n], tok_recv.at[3 + n], to(i, t, sibling))
        for n, g in enumerate((i, other))
    ]

    @pl.when(half != i)
    def _():
        over_dp.start()

    @pl.when(half == i)
    def _():
        over_y[0].start()
        xg[i, my_rows] = scaled

    square_sends = []
    for ds in range(1, 4):
        copy = send(
            squares.at[0], squares.at[ds], sq_send.at[ds], sq_recv.at[ds], to(i, t, lax.rem(s + ds, 4))
        )
        copy.start()
        square_sends.append(copy)

    @pl.when(half != i)
    def _():
        over_y[0].wait_recv()

    over_core[0].start()

    @pl.when(half == i)
    def _():
        over_dp.wait_recv()
        over_y[1].start()

    @pl.when(half != i)
    def _():
        over_y[1].wait_recv()

    over_core[1].start()

    def slab_copy(ds):
        ss = lax.rem(s + ds, 4)
        there = pl.ds(pl.multiple_of(ss * own, 16), own)
        return send(x_t.at[there], slab, slab_send.at[ds], slab_recv, to(i, t, ss))

    @pl.when(s == t)
    def _():
        for ds in range(1, 4):
            slab_copy(ds).start()
        slab[...] = x_t[pl.ds(pl.multiple_of(s * own, 16), own)]

    over_core[1].wait_recv()
    xn[other] = xg[other].T
    part_sends = []
    for k in range(CHUNKS):
        for load in loads[k]:
            load.wait()
        for n, w in enumerate((wg, wu)):
            part_send[k, :, pl.ds(n * ck, ck)] = jnp.dot(
                xn[other], w[k], preferred_element_type=jnp.float32
            ).astype(jnp.bfloat16)
        copy = send(part_send.at[k], part_recv.at[k], part_ssem.at[k], part_rsem.at[k], to(other, t, s))
        copy.start()
        part_sends.append(copy)

    over_core[0].wait_recv()
    xn[i] = xg[i].T
    for k in range(CHUNKS):
        for n, w in enumerate((wg, wu)):
            own_part[k, :, pl.ds(n * ck, ck)] = jnp.dot(xn[i], w[k], preferred_element_type=jnp.float32)
    for copy in square_sends:
        copy.wait()
    total = squares[0] + squares[1] + squares[2] + squares[3]
    inv_row = lax.rsqrt(total[:1] / full + epsilon)
    inv = jnp.broadcast_to(inv_row, (per_device, per_device)).T[:, :1]

    d_sends = []
    for k in range(CHUNKS):
        part_sends[k].wait_recv()
        sums = (own_part[k] + part_recv[k].astype(jnp.float32)) * inv
        gate, up = sums[:, :ck], sums[:, ck:]
        grad = back[k].astype(jnp.float32) * inv
        square = gate * gate
        th = jnp.tanh(SQRT_2_OVER_PI * gate * (1.0 + CUBIC * square))
        cdf = 0.5 * (1.0 + th)
        slope = cdf + 0.5 * gate * (1.0 - th * th) * (SQRT_2_OVER_PI * (1.0 + 3.0 * CUBIC * square))
        d_all[i, k, :, pl.ds(0, ck)] = (grad * up * slope).astype(jnp.bfloat16)
        d_all[i, k, :, pl.ds(ck, ck)] = (grad * gate * cdf).astype(jnp.bfloat16)
        copy = send(d_all.at[i, k], d_all.at[i, k], d_ssem.at[k], d_rsem.at[k], to(other, t, s))
        copy.start()
        d_sends.append(copy)

    piece_sends = []
    for n, g in enumerate((i, other)):
        acc = None
        for k in range(CHUNKS):
            if n == 1:
                d_sends[k].wait_recv()
            for m, w in enumerate((wg, wu)):
                term = lax.dot_general(
                    w[k], d_all[g, k, :, pl.ds(m * ck, ck)], CONTRACT_COLS, preferred_element_type=jnp.float32
                )
                acc = term if acc is None else acc + term
        pieces[n] = acc.astype(jnp.bfloat16)
        for e in range(2):
            tt = 2 * g + lax.rem(t + e, 2)
            dt = lax.rem(tt - t + 4, 4)
            for ds in range(4):
                ss = lax.rem(s + ds, 4)
                r = lax.rem(tt, 2) * 4 + ss
                source = pl.ds(pl.multiple_of(r * own, 16), own)
                slot = dt * 4 + ds
                copy = send(
                    pieces.at[n, source],
                    incoming.at[slot],
                    piece_ssem.at[n, e * 4 + ds],
                    piece_rsem.at[slot],
                    to(i, tt, ss),
                )
                if e == 0 and ds == 0:

                    @pl.when(dt == 0)
                    def _(source=source, n=n):
                        incoming[0] = pieces[n, source]

                    @pl.when(dt != 0)
                    def _(copy=copy):
                        copy.start()

                else:
                    copy.start()
                piece_sends.append((copy, dt, e == 0 and ds == 0))

    for slot in range(1, 16):
        send(
            pieces.at[0, pl.ds(0, own)], incoming.at[slot], piece_ssem.at[0, 0], piece_rsem.at[slot], to(other, t, s)
        ).wait_recv()
    d_sum = incoming[0].astype(jnp.float32)
    for slot in range(1, 16):
        d_sum = d_sum + incoming[slot].astype(jnp.float32)

    move = send(move_send, moved, last_send.at[0], last_recv.at[0], to(other, swap_tp, s))
    moved_f32 = prods.at[0]
    moved_f32[...] = d_sum

    @pl.when(t // 2 != i)
    def _():
        move_send[...] = d_sum.astype(jnp.bfloat16)
        move.start()
        move.wait()
        moved_f32[...] = moved[...].astype(jnp.float32)

    @pl.when(s != t)
    def _():
        slab_copy(1).wait_recv()

    d_own = moved_f32[...]
    mine = slab[...].astype(jnp.float32)
    row_part = jnp.sum(mine * gain_own[...] * d_own, axis=0, keepdims=True)
    rows[0] = jnp.broadcast_to(row_part, rows.shape[1:])
    row_sends = []
    for dt, ds in group:
        slot = dt * 4 + ds
        copy = send(
            rows.at[0],
            rows.at[slot],
            row_ssem.at[slot],
            row_rsem.at[slot],
            to(i, lax.rem(t + dt, 4), lax.rem(s + ds, 4)),
        )
        copy.start()
        row_sends.append(copy)
    prods[1] = mine * d_own
    prod_copy = send(prods.at[1], prods.at[2], last_send.at[1], last_recv.at[1], to(other, t, s))
    prod_copy.start()
    xg_out[...] = xg[...]
    d_out[...] = d_all[...]
    for copy in row_sends:
        copy.wait()
    row_sum = rows[0]
    for slot in range(1, 16):
        row_sum = row_sum + rows[slot]
    factor = inv_row * inv_row * row_sum[:1] / full
    grad_t[...] = (gain_own[...] * d_own - mine * factor).astype(jnp.bfloat16)
    prod_copy.wait()
    prod_out[...] = prods[1] + prods[2]

    @pl.when(half != i)
    def _():
        over_dp.wait_send()

    @pl.when(half == i)
    def _():
        over_y[0].wait_send()
        over_y[1].wait_send()

    @pl.when(s == t)
    def _():
        for ds in range(1, 4):
            slab_copy(ds).wait_send()

    for copy in over_core + part_sends + d_sends:
        copy.wait_send()
    for copy, dt, maybe_self in piece_sends:
        if maybe_self:

            @pl.when(dt != 0)
            def _(copy=copy):
                copy.wait_send()

        else:
            copy.wait_send()


def weight_grad_kernel(xg, d, grad_gate, grad_up):
    features = jnp.concatenate([xg[0], xg[1]], axis=1)
    rows = jnp.concatenate([d[0, 0], d[1, 0]], axis=0)
    ck = grad_gate.shape[1]
    grad_gate[...] = jnp.dot(features, rows[:, :ck], preferred_element_type=jnp.float32).astype(jnp.bfloat16)
    grad_up[...] = jnp.dot(features, rows[:, ck:], preferred_element_type=jnp.float32).astype(jnp.bfloat16)


def fused_shards(tokens, hidden_grad, norm_gain, w_gate, w_up):
    per_device, sec_rows = tokens.shape
    block, width = w_gate.shape
    full = norm_gain.shape[0]
    own = full // 16
    ck = width // CHUNKS
    s = lax.axis_index("section")
    gain_sec = lax.dynamic_slice_in_dim(norm_gain, s * sec_rows, sec_rows, 0)[:, None]
    offset = lax.axis_index(("tp", "section")) * own
    gain_own = lax.dynamic_slice_in_dim(norm_gain, offset, own, 0)[:, None]
    bf, f32 = jnp.bfloat16, jnp.float32
    vmem = pl.BlockSpec(memory_space=pltpu.VMEM)
    anywhere = pl.BlockSpec(memory_space=pl.ANY)
    dma = pltpu.SemaphoreType.DMA
    grad_t, prod, xg, d_all = pl.pallas_call(
        functools.partial(exchange_kernel, full),
        out_shape=(
            jax.ShapeDtypeStruct((own, per_device), bf),
            jax.ShapeDtypeStruct((own, per_device), f32),
            jax.ShapeDtypeStruct((2, block, per_device), bf),
            jax.ShapeDtypeStruct((2, CHUNKS, per_device, 2 * ck), bf),
        ),
        in_specs=[vmem, vmem, vmem, anywhere, anywhere, anywhere],
        out_specs=(vmem, vmem, vmem, vmem),
        scratch_shapes=[
            pltpu.VMEM((CHUNKS, block, ck), bf),
            pltpu.VMEM((CHUNKS, block, ck), bf),
            pltpu.VMEM((CHUNKS, per_device, ck), bf),
            pltpu.VMEM((sec_rows, per_device), bf),
            pltpu.VMEM((2, block, per_device), bf),
            pltpu.VMEM((2, per_device, block), bf),
            pltpu.VMEM((own, per_device), bf),
            pltpu.VMEM((4, 8, per_device), f32),
            pltpu.VMEM((CHUNKS, per_device, 2 * ck), bf),
            pltpu.VMEM((CHUNKS, per_device, 2 * ck), bf),
            pltpu.VMEM((CHUNKS, per_device, 2 * ck), f32),
            pltpu.VMEM((2, CHUNKS, per_device, 2 * ck), bf),
            pltpu.VMEM((2, block, per_device), bf),
            pltpu.VMEM((16, own, per_device), bf),
            pltpu.VMEM((own, per_device), bf),
            pltpu.VMEM((own, per_device), bf),
            pltpu.VMEM((16, 8, per_device), f32),
            pltpu.VMEM((3, own, per_device), f32),
            dma((3, CHUNKS)),
            dma((5,)),
            dma((5,)),
            dma((4,)),
            dma,
            dma((4,)),
            dma((4,)),
            dma((CHUNKS,)),
            dma((CHUNKS,)),
            dma((CHUNKS,)),
            dma((CHUNKS,)),
            dma((2, 8)),
            dma((16,)),
            dma((2,)),
            dma((2,)),
            dma((16,)),
            dma((16,)),
        ],
        compiler_params=pltpu.CompilerParams(
            collective_id=0, has_side_effects=True, vmem_limit_bytes=48 * 1024 * 1024
        ),
    )(tokens.T, gain_sec, gain_own, hidden_grad, w_gate, w_up)
    grad_gate, grad_up = pl.pallas_call(
        weight_grad_kernel,
        grid=(CHUNKS,),
        out_shape=(jax.ShapeDtypeStruct((block, width), bf),) * 2,
        in_specs=[
            pl.BlockSpec((2, block, per_device), lambda k: (0, 0, 0)),
            pl.BlockSpec((2, 1, per_device, 2 * ck), lambda k: (0, k, 0, 0)),
        ],
        out_specs=(pl.BlockSpec((block, ck), lambda k: (0, k)),) * 2,
        compiler_params=pltpu.CompilerParams(vmem_limit_bytes=40 * 1024 * 1024),
    )(xg, d_all)
    return grad_t.T, jnp.sum(prod, axis=1), grad_gate, grad_up


def solution(mesh):
    in_specs = (
        P("dp", "section"),
        P("dp", ("tp", "section")),
        P(),
        P("dp", ("tp", "section")),
        P("dp", ("tp", "section")),
    )
    out_specs = (
        P("dp", ("tp", "section")),
        P(("tp", "section")),
        P("dp", ("tp", "section")),
        P("dp", ("tp", "section")),
    )
    sizes = tuple(mesh.shape[a] for a in ("dp", "tp", "section"))
    body = fused_shards if sizes == (2, 4, 4) else shards
    return jax.shard_map(body, mesh=mesh, in_specs=in_specs, out_specs=out_specs, check_vma=False)
```

```python
import functools

import jax
import jax.numpy as jnp
from jax import lax
from jax.experimental import pallas as pl
from jax.experimental.pallas import tpu as pltpu
from jax.sharding import PartitionSpec as P

D = 2304


epsilon = 1e-06


def gated_unit(gate, up):
    return jax.nn.gelu(gate, approximate=True) * up


def shards(tokens, hidden_grad, norm_gain, w_gate, w_up):
    n_dp = lax.axis_size("dp")
    n_model = lax.axis_size(("tp", "section"))
    rows_in = lax.all_gather(tokens, "section", axis=1, tiled=True)
    inputs = rows_in.astype(jnp.float32)
    inv_rms = lax.rsqrt(jnp.mean(inputs * inputs, axis=1) + epsilon)
    normed = (inputs * inv_rms[:, None] * norm_gain).astype(jnp.bfloat16)
    per_device, features = normed.shape
    cols_normed = lax.all_to_all(normed, "dp", split_axis=1, concat_axis=0, tiled=True)
    width = w_gate.shape[1]
    part_gate = jnp.dot(cols_normed, w_gate, preferred_element_type=jnp.float32)
    part_up = jnp.dot(cols_normed, w_up, preferred_element_type=jnp.float32)
    parts = jnp.concatenate([part_gate, part_up], axis=1).astype(jnp.bfloat16)
    parts = lax.all_to_all(parts, "dp", split_axis=0, concat_axis=0, tiled=True)
    sums = jnp.sum(parts.reshape(n_dp, per_device, 2 * width).astype(jnp.float32), axis=0)
    gate, up = sums[:, :width], sums[:, width:]
    hidden, pull = jax.vjp(gated_unit, gate, up)
    d_both = jnp.concatenate(pull(hidden_grad.astype(jnp.float32)), axis=1).astype(jnp.bfloat16)
    d_all = lax.all_gather(d_both, "dp", axis=0, tiled=True)
    d_gate, d_up = d_all[:, :width], d_all[:, width:]
    contract_cols = (((1,), (1,)), ((), ()))
    contract_rows = (((0,), (0,)), ((), ()))
    first = lax.dot_general(w_gate, d_gate, contract_cols, preferred_element_type=jnp.float32)
    second = lax.dot_general(w_up, d_up, contract_cols, preferred_element_type=jnp.float32)
    own_width = features // n_model
    per_row = n_model // n_dp
    d_part = (first + second).astype(jnp.bfloat16)
    d_part = d_part.reshape(per_row, own_width, n_dp, per_device).transpose(2, 0, 1, 3)
    d_part = d_part.reshape(n_model * own_width, per_device)
    d_columns = lax.psum_scatter(d_part, ("tp", "section"), scatter_dimension=0, tiled=True)
    moves = [
        (i * n_model + o * per_row + r, o * n_model + i * per_row + r)
        for i in range(n_dp)
        for o in range(n_dp)
        for r in range(per_row)
    ]
    d_columns = lax.ppermute(d_columns, ("dp", "tp", "section"), moves)
    d_normed = d_columns.astype(jnp.float32).T
    offset = lax.axis_index(("tp", "section")) * own_width
    own_inputs = lax.dynamic_slice_in_dim(inputs, offset, own_width, 1)
    own_gain = lax.dynamic_slice_in_dim(norm_gain, offset, own_width, 0)
    gain_part = jnp.sum(d_normed * own_inputs * inv_rms[:, None], axis=0)
    row_part = jnp.sum(own_inputs * own_gain * d_normed, axis=1)
    grad_gain = lax.psum(gain_part, "dp")
    row_sum = lax.psum(row_part, ("tp", "section"))
    grad_tokens = (
        inv_rms[:, None] * own_gain * d_normed
        - own_inputs * (inv_rms**3 * row_sum / features)[:, None]
    )
    grad_gate = lax.dot_general(cols_normed, d_gate, contract_rows, preferred_element_type=jnp.float32)
    grad_up = lax.dot_general(cols_normed, d_up, contract_rows, preferred_element_type=jnp.float32)
    return (
        grad_tokens.astype(jnp.bfloat16),
        grad_gain,
        grad_gate.astype(jnp.bfloat16),
        grad_up.astype(jnp.bfloat16),
    )


MESH = pl.DeviceIdType.MESH
SQRT_2_OVER_PI = 0.7978845608028654
CUBIC = 0.044715
CHUNKS = 3
CONTRACT_COLS = (((1,), (1,)), ((), ()))


def exchange_kernel(
    full,
    x_t,
    gain_sec,
    gain_own,
    back_hbm,
    wg_hbm,
    wu_hbm,
    grad_t,
    gain_out,
    xg_out,
    d_out,
    wg,
    wu,
    back,
    xg_send,
    xg,
    xn,
    slab,
    squares,
    part_send,
    part_recv,
    own_part,
    d_all,
    pieces,
    incoming,
    moved,
    move_send,
    rows,
    prods,
    gains,
    sib_in,
    halved,
    load_sem,
    tok_send,
    tok_recv,
    slab_send,
    slab_recv,
    sq_send,
    sq_recv,
    part_ssem,
    part_rsem,
    d_ssem,
    d_rsem,
    piece_ssem,
    piece_rsem,
    sib_ssem,
    sib_rsem,
    last_send,
    last_recv,
    row_ssem,
    row_rsem,
):
    i, t, s = lax.axis_index("dp"), lax.axis_index("tp"), lax.axis_index("section")
    other = 1 - i
    sec_rows, per_device = x_t.shape
    own = slab.shape[0]
    half, q = s // 2, lax.rem(s, 2)
    sibling, across = s + 1 - 2 * q, s + 2 - 4 * half
    ck = wg.shape[2]
    width = CHUNKS * ck

    def to(d, tt, ss):
        return {"dp": d, "tp": tt, "section": ss}

    def send(src, dst, ssem, rsem, target):
        return pltpu.make_async_remote_copy(
            src_ref=src, dst_ref=dst, send_sem=ssem, recv_sem=rsem, device_id=target, device_id_type=MESH
        )

    barrier = pltpu.get_barrier_semaphore()
    group = [(dt, ds) for dt in range(4) for ds in range(4) if dt + ds > 0]
    swap_tp = t + 2 - 4 * (t // 2)
    everyone = [to(i, lax.rem(t + dt, 4), lax.rem(s + ds, 4)) for dt, ds in group]
    everyone += [to(other, t, s), to(other, swap_tp, s)]
    for target in everyone:
        pl.semaphore_signal(barrier, inc=1, device_id=target, device_id_type=MESH)

    loads = []
    for k in range(CHUNKS):
        cols = pl.ds(k * ck, ck)
        loads.append(
            (
                pltpu.make_async_copy(wg_hbm.at[:, cols], wg.at[k], load_sem.at[0, k]),
                pltpu.make_async_copy(wu_hbm.at[:, cols], wu.at[k], load_sem.at[1, k]),
                pltpu.make_async_copy(back_hbm.at[:, cols], back.at[k], load_sem.at[2, k]),
            )
        )
        for load in loads[-1]:
            load.start()

    raw = x_t[...].astype(jnp.float32)
    scaled = (raw * gain_sec[...]).astype(jnp.bfloat16)
    xg_send[...] = scaled
    squares[0] = jnp.broadcast_to(jnp.sum(raw * raw, axis=0, keepdims=True), squares.shape[1:])
    my_rows = pl.ds(pl.multiple_of(q * sec_rows, 16), sec_rows)

    pl.semaphore_wait(barrier, len(everyone))

    over_dp = send(xg_send, xg.at[i, my_rows], tok_send.at[0], tok_recv.at[0], to(other, t, s))
    over_y = [
        send(xg_send, xg.at[i, my_rows], tok_send.at[1], tok_recv.at[1], to(i, t, across)),
        send(xg.at[other, my_rows], xg.at[other, my_rows], tok_send.at[2], tok_recv.at[2], to(i, t, across)),
    ]
    over_core = [
        send(xg.at[g, my_rows], xg.at[g, my_rows], tok_send.at[3 + n], tok_recv.at[3 + n], to(i, t, sibling))
        for n, g in enumerate((i, other))
    ]

    @pl.when(half != i)
    def _():
        over_dp.start()

    @pl.when(half == i)
    def _():
        over_y[0].start()
        xg[i, my_rows] = scaled

    square_sends = []
    for ds in range(1, 4):
        copy = send(
            squares.at[0], squares.at[ds], sq_send.at[ds], sq_recv.at[ds], to(i, t, lax.rem(s + ds, 4))
        )
        copy.start()
        square_sends.append(copy)

    @pl.when(half != i)
    def _():
        over_y[0].wait_recv()

    over_core[0].start()

    @pl.when(half == i)
    def _():
        over_dp.wait_recv()
        over_y[1].start()

    @pl.when(half != i)
    def _():
        over_y[1].wait_recv()

    over_core[1].start()

    def slab_copy(ds):
        ss = lax.rem(s + ds, 4)
        there = pl.ds(pl.multiple_of(ss * own, 16), own)
        return send(x_t.at[there], slab, slab_send.at[ds], slab_recv, to(i, t, ss))

    @pl.when(s == t)
    def _():
        for ds in range(1, 4):
            slab_copy(ds).start()
        slab[...] = x_t[pl.ds(pl.multiple_of(s * own, 16), own)]

    over_core[1].wait_recv()
    xn[other] = xg[other].T
    part_sends = []
    for k in range(CHUNKS):
        for load in loads[k]:
            load.wait()
        for n, w in enumerate((wg, wu)):
            part_send[k, :, pl.ds(n * ck, ck)] = jnp.dot(
                xn[other], w[k], preferred_element_type=jnp.float32
            ).astype(jnp.bfloat16)
        copy = send(part_send.at[k], part_recv.at[k], part_ssem.at[k], part_rsem.at[k], to(other, t, s))
        copy.start()
        part_sends.append(copy)

    over_core[0].wait_recv()
    xn[i] = xg[i].T
    for k in range(CHUNKS):
        for n, w in enumerate((wg, wu)):
            own_part[k, :, pl.ds(n * ck, ck)] = jnp.dot(xn[i], w[k], preferred_element_type=jnp.float32)
    for copy in square_sends:
        copy.wait()
    total = squares[0] + squares[1] + squares[2] + squares[3]
    inv_row = lax.rsqrt(total[:1] / full + epsilon)
    inv = jnp.broadcast_to(inv_row, (per_device, per_device)).T[:, :1]

    d_sends = []
    row_col = jnp.zeros((per_device, 1), jnp.float32)
    for k in range(CHUNKS):
        part_sends[k].wait_recv()
        raw_sums = own_part[k] + part_recv[k].astype(jnp.float32)
        gate, up = raw_sums[:, :ck] * inv, raw_sums[:, ck:] * inv
        grad = back[k].astype(jnp.float32) * inv
        square = gate * gate
        th = jnp.tanh(SQRT_2_OVER_PI * gate * (1.0 + CUBIC * square))
        cdf = 0.5 * (1.0 + th)
        slope = cdf + 0.5 * gate * (1.0 - th * th) * (SQRT_2_OVER_PI * (1.0 + 3.0 * CUBIC * square))
        d_gate, d_up = grad * up * slope, grad * gate * cdf
        d_all[i, k, :, pl.ds(0, ck)] = d_gate.astype(jnp.bfloat16)
        d_all[i, k, :, pl.ds(ck, ck)] = d_up.astype(jnp.bfloat16)
        copy = send(d_all.at[i, k], d_all.at[i, k], d_ssem.at[k], d_rsem.at[k], to(other, t, s))
        copy.start()
        d_sends.append(copy)
        terms = d_gate * raw_sums[:, :ck] + d_up * raw_sums[:, ck:]
        row_col = row_col + jnp.sum(terms, axis=1, keepdims=True)

    rows[0] = jnp.broadcast_to(row_col, (per_device, per_device)).T[:8]
    row_sends = []
    for dt, ds in group:
        slot = dt * 4 + ds
        copy = send(
            rows.at[0],
            rows.at[slot],
            row_ssem.at[slot],
            row_rsem.at[slot],
            to(i, lax.rem(t + dt, 4), lax.rem(s + ds, 4)),
        )
        copy.start()
        row_sends.append(copy)

    piece_sends = []
    for n, g in enumerate((i, other)):
        acc = None
        for k in range(CHUNKS):
            if n == 1:
                d_sends[k].wait_recv()
            for m, w in enumerate((wg, wu)):
                term = lax.dot_general(
                    w[k], d_all[g, k, :, pl.ds(m * ck, ck)], CONTRACT_COLS, preferred_element_type=jnp.float32
                )
                acc = term if acc is None else acc + term
        for r in range(8):
            pieces[n, r // 2, r % 2] = acc[r * own : (r + 1) * own].astype(jnp.bfloat16)
        swap = send(
            pieces.at[n, :, 1 - q], sib_in.at[n], sib_ssem.at[n], sib_rsem.at[n], to(i, t, sibling)
        )
        swap.start()
        swap.wait_recv()
        for r in range(4):
            halved[n, r] = (
                pieces[n, r, q].astype(jnp.float32) + sib_in[n, r].astype(jnp.float32)
            ).astype(jnp.bfloat16)
        piece_sends.append((swap, None, False))
        for e in (1, 0):
            tt = 2 * g + lax.rem(t + e, 2)
            dt = lax.rem(tt - t + 4, 4)
            for dy in (1, 0):
                ss = across if dy else s
                r = lax.rem(tt, 2) * 2 + ss // 2
                slot = dt * 2 + dy
                copy = send(
                    halved.at[n, r],
                    incoming.at[slot],
                    piece_ssem.at[n, e * 2 + dy],
                    piece_rsem.at[slot],
                    to(i, tt, ss),
                )
                maybe_self = e == 0 and dy == 0
                if maybe_self:

                    @pl.when(dt == 0)
                    def _(r=r, n=n):
                        incoming[0] = halved[n, r]

                    @pl.when(dt != 0)
                    def _(copy=copy):
                        copy.start()

                else:
                    copy.start()
                piece_sends.append((copy, dt, maybe_self))

    xg_out[...] = xg[...]
    d_out[...] = d_all[...]
    for copy in row_sends:
        copy.wait()

    for slot in range(1, 8):
        send(
            halved.at[0, 0], incoming.at[slot], piece_ssem.at[0, 0], piece_rsem.at[slot], to(other, t, s)
        ).wait_recv()
    d_sum = incoming[0].astype(jnp.float32)
    for slot in range(1, 8):
        d_sum = d_sum + incoming[slot].astype(jnp.float32)

    move = send(move_send, moved, last_send.at[0], last_recv.at[0], to(other, swap_tp, s))
    moved_f32 = prods.at[1, pl.ds(0, own)]
    moved_f32[...] = d_sum

    @pl.when(t // 2 != i)
    def _():
        move_send[...] = d_sum.astype(jnp.bfloat16)
        move.start()
        move.wait()
        moved_f32[...] = moved[...].astype(jnp.float32)

    @pl.when(s != t)
    def _():
        slab_copy(1).wait_recv()

    d_own = moved_f32[...]
    mine = slab[...].astype(jnp.float32)
    prods[0] = jnp.zeros(prods.shape[1:], jnp.float32)
    prods[0, pl.ds(0, own)] = mine * d_own
    gains[0] = jnp.broadcast_to(jnp.sum(prods[0].T, axis=0, keepdims=True), gains.shape[1:])
    gain_copy = send(gains.at[0], gains.at[1], last_send.at[1], last_recv.at[1], to(other, t, s))
    gain_copy.start()
    row_sum = rows[0]
    for slot in range(1, 16):
        row_sum = row_sum + rows[slot]
    factor = inv_row * inv_row * row_sum[:1] / full
    grad_t[...] = (gain_own[...] * d_own - mine * factor).astype(jnp.bfloat16)
    gain_copy.wait()
    gain_out[...] = gains[0] + gains[1]

    @pl.when(half != i)
    def _():
        over_dp.wait_send()

    @pl.when(half == i)
    def _():
        over_y[0].wait_send()
        over_y[1].wait_send()

    @pl.when(s == t)
    def _():
        for ds in range(1, 4):
            slab_copy(ds).wait_send()

    for copy in over_core + part_sends + d_sends:
        copy.wait_send()
    for copy, dt, maybe_self in piece_sends:
        if maybe_self:

            @pl.when(dt != 0)
            def _(copy=copy):
                copy.wait_send()

        else:
            copy.wait_send()


def weight_grad_kernel(xg, d, grad_gate, grad_up):
    features = jnp.concatenate([xg[0], xg[1]], axis=1)
    rows = jnp.concatenate([d[0, 0], d[1, 0]], axis=0)
    ck = grad_gate.shape[1]
    grad_gate[...] = jnp.dot(features, rows[:, :ck], preferred_element_type=jnp.float32).astype(jnp.bfloat16)
    grad_up[...] = jnp.dot(features, rows[:, ck:], preferred_element_type=jnp.float32).astype(jnp.bfloat16)


def fused_shards(tokens, hidden_grad, norm_gain, w_gate, w_up):
    per_device, sec_rows = tokens.shape
    block, width = w_gate.shape
    full = norm_gain.shape[0]
    own = full // 16
    ck = width // CHUNKS
    s = lax.axis_index("section")
    gain_sec = lax.dynamic_slice_in_dim(norm_gain, s * sec_rows, sec_rows, 0)[:, None]
    offset = lax.axis_index(("tp", "section")) * own
    gain_own = lax.dynamic_slice_in_dim(norm_gain, offset, own, 0)[:, None]
    bf, f32 = jnp.bfloat16, jnp.float32
    vmem = pl.BlockSpec(memory_space=pltpu.VMEM)
    anywhere = pl.BlockSpec(memory_space=pl.ANY)
    dma = pltpu.SemaphoreType.DMA
    own_pad = pl.cdiv(own, 128) * 128
    grad_t, gain_sum, xg, d_all = pl.pallas_call(
        functools.partial(exchange_kernel, full),
        out_shape=(
            jax.ShapeDtypeStruct((own, per_device), bf),
            jax.ShapeDtypeStruct((8, own_pad), f32),
            jax.ShapeDtypeStruct((2, block, per_device), bf),
            jax.ShapeDtypeStruct((2, CHUNKS, per_device, 2 * ck), bf),
        ),
        in_specs=[vmem, vmem, vmem, anywhere, anywhere, anywhere],
        out_specs=(vmem, vmem, vmem, vmem),
        scratch_shapes=[
            pltpu.VMEM((CHUNKS, block, ck), bf),
            pltpu.VMEM((CHUNKS, block, ck), bf),
            pltpu.VMEM((CHUNKS, per_device, ck), bf),
            pltpu.VMEM((sec_rows, per_device), bf),
            pltpu.VMEM((2, block, per_device), bf),
            pltpu.VMEM((2, per_device, block), bf),
            pltpu.VMEM((own, per_device), bf),
            pltpu.VMEM((4, 8, per_device), f32),
            pltpu.VMEM((CHUNKS, per_device, 2 * ck), bf),
            pltpu.VMEM((CHUNKS, per_device, 2 * ck), bf),
            pltpu.VMEM((CHUNKS, per_device, 2 * ck), f32),
            pltpu.VMEM((2, CHUNKS, per_device, 2 * ck), bf),
            pltpu.VMEM((2, 4, 2, own, per_device), bf),
            pltpu.VMEM((8, own, per_device), bf),
            pltpu.VMEM((own, per_device), bf),
            pltpu.VMEM((own, per_device), bf),
            pltpu.VMEM((16, 8, per_device), f32),
            pltpu.VMEM((2, own_pad, per_device), f32),
            pltpu.VMEM((2, 8, own_pad), f32),
            pltpu.VMEM((2, 4, own, per_device), bf),
            pltpu.VMEM((2, 4, own, per_device), bf),
            dma((3, CHUNKS)),
            dma((5,)),
            dma((5,)),
            dma((4,)),
            dma,
            dma((4,)),
            dma((4,)),
            dma((CHUNKS,)),
            dma((CHUNKS,)),
            dma((CHUNKS,)),
            dma((CHUNKS,)),
            dma((2, 4)),
            dma((8,)),
            dma((2,)),
            dma((2,)),
            dma((2,)),
            dma((2,)),
            dma((16,)),
            dma((16,)),
        ],
        compiler_params=pltpu.CompilerParams(
            collective_id=0, has_side_effects=True, vmem_limit_bytes=60 * 1024 * 1024
        ),
    )(tokens.T, gain_sec, gain_own, hidden_grad, w_gate, w_up)
    grad_gate, grad_up = pl.pallas_call(
        weight_grad_kernel,
        grid=(CHUNKS,),
        out_shape=(jax.ShapeDtypeStruct((block, width), bf),) * 2,
        in_specs=[
            pl.BlockSpec((2, block, per_device), lambda k: (0, 0, 0)),
            pl.BlockSpec((2, 1, per_device, 2 * ck), lambda k: (0, k, 0, 0)),
        ],
        out_specs=(pl.BlockSpec((block, ck), lambda k: (0, k)),) * 2,
        compiler_params=pltpu.CompilerParams(vmem_limit_bytes=60 * 1024 * 1024),
    )(xg, d_all)
    return grad_t.T, gain_sum[0, :own], grad_gate, grad_up


def solution(mesh):
    in_specs = (
        P("dp", "section"),
        P("dp", ("tp", "section")),
        P(),
        P("dp", ("tp", "section")),
        P("dp", ("tp", "section")),
    )
    out_specs = (
        P("dp", ("tp", "section")),
        P(("tp", "section")),
        P("dp", ("tp", "section")),
        P("dp", ("tp", "section")),
    )
    sizes = tuple(mesh.shape[a] for a in ("dp", "tp", "section"))
    body = fused_shards if sizes == (2, 4, 4) else shards
    return jax.shard_map(body, mesh=mesh, in_specs=in_specs, out_specs=out_specs, check_vma=False)
```

```python
import functools

import jax
import jax.numpy as jnp
from jax import lax
from jax.experimental import pallas as pl
from jax.experimental.pallas import tpu as pltpu
from jax.sharding import PartitionSpec as P

D = 2304


epsilon = 1e-06


def gated_unit(gate, up):
    return jax.nn.gelu(gate, approximate=True) * up


def shards(tokens, hidden_grad, norm_gain, w_gate, w_up):
    n_dp = lax.axis_size("dp")
    n_model = lax.axis_size(("tp", "section"))
    rows_in = lax.all_gather(tokens, "section", axis=1, tiled=True)
    inputs = rows_in.astype(jnp.float32)
    inv_rms = lax.rsqrt(jnp.mean(inputs * inputs, axis=1) + epsilon)
    normed = (inputs * inv_rms[:, None] * norm_gain).astype(jnp.bfloat16)
    per_device, features = normed.shape
    cols_normed = lax.all_to_all(normed, "dp", split_axis=1, concat_axis=0, tiled=True)
    width = w_gate.shape[1]
    part_gate = jnp.dot(cols_normed, w_gate, preferred_element_type=jnp.float32)
    part_up = jnp.dot(cols_normed, w_up, preferred_element_type=jnp.float32)
    parts = jnp.concatenate([part_gate, part_up], axis=1).astype(jnp.bfloat16)
    parts = lax.all_to_all(parts, "dp", split_axis=0, concat_axis=0, tiled=True)
    sums = jnp.sum(parts.reshape(n_dp, per_device, 2 * width).astype(jnp.float32), axis=0)
    gate, up = sums[:, :width], sums[:, width:]
    hidden, pull = jax.vjp(gated_unit, gate, up)
    d_both = jnp.concatenate(pull(hidden_grad.astype(jnp.float32)), axis=1).astype(jnp.bfloat16)
    d_all = lax.all_gather(d_both, "dp", axis=0, tiled=True)
    d_gate, d_up = d_all[:, :width], d_all[:, width:]
    contract_cols = (((1,), (1,)), ((), ()))
    contract_rows = (((0,), (0,)), ((), ()))
    first = lax.dot_general(w_gate, d_gate, contract_cols, preferred_element_type=jnp.float32)
    second = lax.dot_general(w_up, d_up, contract_cols, preferred_element_type=jnp.float32)
    own_width = features // n_model
    per_row = n_model // n_dp
    d_part = (first + second).astype(jnp.bfloat16)
    d_part = d_part.reshape(per_row, own_width, n_dp, per_device).transpose(2, 0, 1, 3)
    d_part = d_part.reshape(n_model * own_width, per_device)
    d_columns = lax.psum_scatter(d_part, ("tp", "section"), scatter_dimension=0, tiled=True)
    moves = [
        (i * n_model + o * per_row + r, o * n_model + i * per_row + r)
        for i in range(n_dp)
        for o in range(n_dp)
        for r in range(per_row)
    ]
    d_columns = lax.ppermute(d_columns, ("dp", "tp", "section"), moves)
    d_normed = d_columns.astype(jnp.float32).T
    offset = lax.axis_index(("tp", "section")) * own_width
    own_inputs = lax.dynamic_slice_in_dim(inputs, offset, own_width, 1)
    own_gain = lax.dynamic_slice_in_dim(norm_gain, offset, own_width, 0)
    gain_part = jnp.sum(d_normed * own_inputs * inv_rms[:, None], axis=0)
    row_part = jnp.sum(own_inputs * own_gain * d_normed, axis=1)
    grad_gain = lax.psum(gain_part, "dp")
    row_sum = lax.psum(row_part, ("tp", "section"))
    grad_tokens = (
        inv_rms[:, None] * own_gain * d_normed
        - own_inputs * (inv_rms**3 * row_sum / features)[:, None]
    )
    grad_gate = lax.dot_general(cols_normed, d_gate, contract_rows, preferred_element_type=jnp.float32)
    grad_up = lax.dot_general(cols_normed, d_up, contract_rows, preferred_element_type=jnp.float32)
    return (
        grad_tokens.astype(jnp.bfloat16),
        grad_gain,
        grad_gate.astype(jnp.bfloat16),
        grad_up.astype(jnp.bfloat16),
    )


MESH = pl.DeviceIdType.MESH
SQRT_2_OVER_PI = 0.7978845608028654
CUBIC = 0.044715
CHUNKS = 3
CONTRACT_COLS = (((1,), (1,)), ((), ()))


def exchange_kernel(
    full,
    x_t,
    gain,
    back_hbm,
    wg_hbm,
    wu_hbm,
    grad_t,
    gain_out,
    xg_out,
    d_out,
    wg,
    wu,
    back,
    xg_send,
    xg,
    xn,
    slab,
    squares,
    part_send,
    part_recv,
    own_part,
    d_all,
    pieces,
    incoming,
    moved,
    move_send,
    rows,
    prods,
    gains,
    sib_in,
    halved,
    load_sem,
    tok_send,
    tok_recv,
    slab_send,
    slab_recv,
    sq_send,
    sq_recv,
    part_ssem,
    part_rsem,
    d_ssem,
    d_rsem,
    piece_ssem,
    piece_rsem,
    sib_ssem,
    sib_rsem,
    last_send,
    last_recv,
    row_ssem,
    row_rsem,
):
    i, t, s = lax.axis_index("dp"), lax.axis_index("tp"), lax.axis_index("section")
    other = 1 - i
    sec_rows, per_device = x_t.shape
    own = slab.shape[0]
    gain_own = gain.at[pl.ds(pl.multiple_of((t * 4 + s) * own, 16), own)]
    half, q = s // 2, lax.rem(s, 2)
    sibling, across = s + 1 - 2 * q, s + 2 - 4 * half
    ck = wg.shape[2]
    width = CHUNKS * ck

    def to(d, tt, ss):
        return {"dp": d, "tp": tt, "section": ss}

    def send(src, dst, ssem, rsem, target):
        return pltpu.make_async_remote_copy(
            src_ref=src, dst_ref=dst, send_sem=ssem, recv_sem=rsem, device_id=target, device_id_type=MESH
        )

    barrier = pltpu.get_barrier_semaphore()
    group = [(dt, ds) for dt in range(4) for ds in range(4) if dt + ds > 0]
    swap_tp = t + 2 - 4 * (t // 2)
    everyone = [to(i, lax.rem(t + dt, 4), lax.rem(s + ds, 4)) for dt, ds in group]
    everyone += [to(other, t, s), to(other, swap_tp, s)]
    for target in everyone:
        pl.semaphore_signal(barrier, inc=1, device_id=target, device_id_type=MESH)

    loads = []
    for k in range(CHUNKS):
        cols = pl.ds(k * ck, ck)
        loads.append(
            (
                pltpu.make_async_copy(wg_hbm.at[:, cols], wg.at[k], load_sem.at[0, k]),
                pltpu.make_async_copy(wu_hbm.at[:, cols], wu.at[k], load_sem.at[1, k]),
                pltpu.make_async_copy(back_hbm.at[:, cols], back.at[k], load_sem.at[2, k]),
            )
        )
        for load in loads[-1]:
            load.start()

    raw = x_t[...].astype(jnp.float32)
    scaled = (raw * gain[pl.ds(pl.multiple_of(s * sec_rows, 16), sec_rows)]).astype(jnp.bfloat16)
    xg_send[...] = scaled
    squares[0] = jnp.broadcast_to(jnp.sum(raw * raw, axis=0, keepdims=True), squares.shape[1:])
    my_rows = pl.ds(pl.multiple_of(q * sec_rows, 16), sec_rows)

    pl.semaphore_wait(barrier, len(everyone))

    over_dp = send(xg_send, xg.at[i, my_rows], tok_send.at[0], tok_recv.at[0], to(other, t, s))
    over_y = [
        send(xg_send, xg.at[i, my_rows], tok_send.at[1], tok_recv.at[1], to(i, t, across)),
        send(xg.at[other, my_rows], xg.at[other, my_rows], tok_send.at[2], tok_recv.at[2], to(i, t, across)),
    ]
    over_core = [
        send(xg.at[g, my_rows], xg.at[g, my_rows], tok_send.at[3 + n], tok_recv.at[3 + n], to(i, t, sibling))
        for n, g in enumerate((i, other))
    ]

    @pl.when(half != i)
    def _():
        over_dp.start()

    @pl.when(half == i)
    def _():
        over_y[0].start()
        xg[i, my_rows] = scaled

    square_sends = []
    for ds in range(1, 4):
        copy = send(
            squares.at[0], squares.at[ds], sq_send.at[ds], sq_recv.at[ds], to(i, t, lax.rem(s + ds, 4))
        )
        copy.start()
        square_sends.append(copy)

    @pl.when(half != i)
    def _():
        over_y[0].wait_recv()

    over_core[0].start()

    @pl.when(half == i)
    def _():
        over_dp.wait_recv()
        over_y[1].start()

    @pl.when(half != i)
    def _():
        over_y[1].wait_recv()

    over_core[1].start()

    def slab_copy(ds):
        ss = lax.rem(s + ds, 4)
        there = pl.ds(pl.multiple_of(ss * own, 16), own)
        return send(x_t.at[there], slab, slab_send.at[ds], slab_recv, to(i, t, ss))

    @pl.when(s == t)
    def _():
        for ds in range(1, 4):
            slab_copy(ds).start()
        slab[...] = x_t[pl.ds(pl.multiple_of(s * own, 16), own)]

    over_core[1].wait_recv()
    xn[other] = xg[other].T
    part_sends = []
    for k in range(CHUNKS):
        for load in loads[k]:
            load.wait()
        for n, w in enumerate((wg, wu)):
            part_send[k, :, pl.ds(n * ck, ck)] = jnp.dot(
                xn[other], w[k], preferred_element_type=jnp.float32
            ).astype(jnp.bfloat16)
        copy = send(part_send.at[k], part_recv.at[k], part_ssem.at[k], part_rsem.at[k], to(other, t, s))
        copy.start()
        part_sends.append(copy)

    over_core[0].wait_recv()
    xn[i] = xg[i].T
    for k in range(CHUNKS):
        for n, w in enumerate((wg, wu)):
            own_part[k, :, pl.ds(n * ck, ck)] = jnp.dot(xn[i], w[k], preferred_element_type=jnp.float32)
    for copy in square_sends:
        copy.wait()
    total = squares[0] + squares[1] + squares[2] + squares[3]
    inv_row = lax.rsqrt(total[:1] / full + epsilon)
    inv = jnp.broadcast_to(inv_row, (per_device, per_device)).T[:, :1]

    d_sends = []
    row_col = jnp.zeros((per_device, 1), jnp.float32)
    for k in range(CHUNKS):
        part_sends[k].wait_recv()
        raw_sums = own_part[k] + part_recv[k].astype(jnp.float32)
        gate, up = raw_sums[:, :ck] * inv, raw_sums[:, ck:] * inv
        grad = back[k].astype(jnp.float32) * inv
        square = gate * gate
        th = jnp.tanh(SQRT_2_OVER_PI * gate * (1.0 + CUBIC * square))
        cdf = 0.5 * (1.0 + th)
        slope = cdf + 0.5 * gate * (1.0 - th * th) * (SQRT_2_OVER_PI * (1.0 + 3.0 * CUBIC * square))
        d_gate, d_up = grad * up * slope, grad * gate * cdf
        d_all[i, k, :, pl.ds(0, ck)] = d_gate.astype(jnp.bfloat16)
        d_all[i, k, :, pl.ds(ck, ck)] = d_up.astype(jnp.bfloat16)
        copy = send(d_all.at[i, k], d_all.at[i, k], d_ssem.at[k], d_rsem.at[k], to(other, t, s))
        copy.start()
        d_sends.append(copy)
        terms = d_gate * raw_sums[:, :ck] + d_up * raw_sums[:, ck:]
        row_col = row_col + jnp.sum(terms, axis=1, keepdims=True)

    rows[0] = jnp.broadcast_to(row_col, (per_device, per_device)).T[:8]
    row_sends = []
    for dt, ds in group:
        slot = dt * 4 + ds
        copy = send(
            rows.at[0],
            rows.at[slot],
            row_ssem.at[slot],
            row_rsem.at[slot],
            to(i, lax.rem(t + dt, 4), lax.rem(s + ds, 4)),
        )
        copy.start()
        row_sends.append(copy)

    piece_sends = []
    for n, g in enumerate((i, other)):
        acc = None
        for k in range(CHUNKS):
            if n == 1:
                d_sends[k].wait_recv()
            for m, w in enumerate((wg, wu)):
                term = lax.dot_general(
                    w[k], d_all[g, k, :, pl.ds(m * ck, ck)], CONTRACT_COLS, preferred_element_type=jnp.float32
                )
                acc = term if acc is None else acc + term
        for r in range(8):
            pieces[n, r // 2, r % 2] = acc[r * own : (r + 1) * own].astype(jnp.bfloat16)
        swap = send(
            pieces.at[n, :, 1 - q], sib_in.at[n], sib_ssem.at[n], sib_rsem.at[n], to(i, t, sibling)
        )
        swap.start()
        swap.wait_recv()
        for r in range(4):
            halved[n, r] = (
                pieces[n, r, q].astype(jnp.float32) + sib_in[n, r].astype(jnp.float32)
            ).astype(jnp.bfloat16)
        piece_sends.append((swap, None, False))
        for e in (1, 0):
            tt = 2 * g + lax.rem(t + e, 2)
            dt = lax.rem(tt - t + 4, 4)
            for dy in (1, 0):
                ss = across if dy else s
                r = lax.rem(tt, 2) * 2 + ss // 2
                slot = dt * 2 + dy
                copy = send(
                    halved.at[n, r],
                    incoming.at[slot],
                    piece_ssem.at[n, e * 2 + dy],
                    piece_rsem.at[slot],
                    to(i, tt, ss),
                )
                maybe_self = e == 0 and dy == 0
                if maybe_self:

                    @pl.when(dt == 0)
                    def _(r=r, n=n):
                        incoming[0] = halved[n, r]

                    @pl.when(dt != 0)
                    def _(copy=copy):
                        copy.start()

                else:
                    copy.start()
                piece_sends.append((copy, dt, maybe_self))

    xg_out[...] = xg[...]
    d_out[...] = d_all[...]
    for copy in row_sends:
        copy.wait()

    for slot in range(1, 8):
        send(
            halved.at[0, 0], incoming.at[slot], piece_ssem.at[0, 0], piece_rsem.at[slot], to(other, t, s)
        ).wait_recv()
    d_sum = incoming[0].astype(jnp.float32)
    for slot in range(1, 8):
        d_sum = d_sum + incoming[slot].astype(jnp.float32)

    move = send(move_send, moved, last_send.at[0], last_recv.at[0], to(other, swap_tp, s))
    moved_f32 = prods.at[1, pl.ds(0, own)]
    moved_f32[...] = d_sum

    @pl.when(t // 2 != i)
    def _():
        move_send[...] = d_sum.astype(jnp.bfloat16)
        move.start()
        move.wait()
        moved_f32[...] = moved[...].astype(jnp.float32)

    @pl.when(s != t)
    def _():
        slab_copy(1).wait_recv()

    d_own = moved_f32[...]
    mine = slab[...].astype(jnp.float32)
    prods[0] = jnp.zeros(prods.shape[1:], jnp.float32)
    prods[0, pl.ds(0, own)] = mine * d_own
    gains[0] = jnp.broadcast_to(jnp.sum(prods[0].T, axis=0, keepdims=True), gains.shape[1:])
    gain_copy = send(gains.at[0], gains.at[1], last_send.at[1], last_recv.at[1], to(other, t, s))
    gain_copy.start()
    row_sum = rows[0]
    for slot in range(1, 16):
        row_sum = row_sum + rows[slot]
    factor = inv_row * inv_row * row_sum[:1] / full
    grad_t[...] = (gain_own[...] * d_own - mine * factor).astype(jnp.bfloat16)
    gain_copy.wait()
    gain_out[...] = gains[0] + gains[1]

    @pl.when(half != i)
    def _():
        over_dp.wait_send()

    @pl.when(half == i)
    def _():
        over_y[0].wait_send()
        over_y[1].wait_send()

    @pl.when(s == t)
    def _():
        for ds in range(1, 4):
            slab_copy(ds).wait_send()

    for copy in over_core + part_sends + d_sends:
        copy.wait_send()
    for copy, dt, maybe_self in piece_sends:
        if maybe_self:

            @pl.when(dt != 0)
            def _(copy=copy):
                copy.wait_send()

        else:
            copy.wait_send()


def weight_grad_kernel(xg, d, grad_gate, grad_up):
    features = jnp.concatenate([xg[0], xg[1]], axis=1)
    rows = jnp.concatenate([d[0, 0], d[1, 0]], axis=0)
    ck = grad_gate.shape[1]
    grad_gate[...] = jnp.dot(features, rows[:, :ck], preferred_element_type=jnp.float32).astype(jnp.bfloat16)
    grad_up[...] = jnp.dot(features, rows[:, ck:], preferred_element_type=jnp.float32).astype(jnp.bfloat16)


def fused_shards(tokens, hidden_grad, norm_gain, w_gate, w_up):
    per_device, sec_rows = tokens.shape
    block, width = w_gate.shape
    full = norm_gain.shape[0]
    own = full // 16
    ck = width // CHUNKS
    bf, f32 = jnp.bfloat16, jnp.float32
    vmem = pl.BlockSpec(memory_space=pltpu.VMEM)
    anywhere = pl.BlockSpec(memory_space=pltpu.HBM)
    dma = pltpu.SemaphoreType.DMA
    own_pad = pl.cdiv(own, 128) * 128
    grad_t, gain_sum, xg, d_all = pl.pallas_call(
        functools.partial(exchange_kernel, full),
        out_shape=(
            jax.ShapeDtypeStruct((own, per_device), bf),
            jax.ShapeDtypeStruct((8, own_pad), f32),
            jax.ShapeDtypeStruct((2, block, per_device), bf),
            jax.ShapeDtypeStruct((2, CHUNKS, per_device, 2 * ck), bf),
        ),
        in_specs=[vmem, vmem, anywhere, anywhere, anywhere],
        out_specs=(vmem, vmem, vmem, vmem),
        scratch_shapes=[
            pltpu.VMEM((CHUNKS, block, ck), bf),
            pltpu.VMEM((CHUNKS, block, ck), bf),
            pltpu.VMEM((CHUNKS, per_device, ck), bf),
            pltpu.VMEM((sec_rows, per_device), bf),
            pltpu.VMEM((2, block, per_device), bf),
            pltpu.VMEM((2, per_device, block), bf),
            pltpu.VMEM((own, per_device), bf),
            pltpu.VMEM((4, 8, per_device), f32),
            pltpu.VMEM((CHUNKS, per_device, 2 * ck), bf),
            pltpu.VMEM((CHUNKS, per_device, 2 * ck), bf),
            pltpu.VMEM((CHUNKS, per_device, 2 * ck), f32),
            pltpu.VMEM((2, CHUNKS, per_device, 2 * ck), bf),
            pltpu.VMEM((2, 4, 2, own, per_device), bf),
            pltpu.VMEM((8, own, per_device), bf),
            pltpu.VMEM((own, per_device), bf),
            pltpu.VMEM((own, per_device), bf),
            pltpu.VMEM((16, 8, per_device), f32),
            pltpu.VMEM((2, own_pad, per_device), f32),
            pltpu.VMEM((2, 8, own_pad), f32),
            pltpu.VMEM((2, 4, own, per_device), bf),
            pltpu.VMEM((2, 4, own, per_device), bf),
            dma((3, CHUNKS)),
            dma((5,)),
            dma((5,)),
            dma((4,)),
            dma,
            dma((4,)),
            dma((4,)),
            dma((CHUNKS,)),
            dma((CHUNKS,)),
            dma((CHUNKS,)),
            dma((CHUNKS,)),
            dma((2, 4)),
            dma((8,)),
            dma((2,)),
            dma((2,)),
            dma((2,)),
            dma((2,)),
            dma((16,)),
            dma((16,)),
        ],
        compiler_params=pltpu.CompilerParams(
            collective_id=0, has_side_effects=True, vmem_limit_bytes=51 * 1024 * 1024
        ),
    )(tokens.T, norm_gain[:, None], hidden_grad, w_gate, w_up)
    grad_gate, grad_up = pl.pallas_call(
        weight_grad_kernel,
        grid=(CHUNKS,),
        out_shape=(jax.ShapeDtypeStruct((block, width), bf),) * 2,
        in_specs=[
            pl.BlockSpec((2, block, per_device), lambda k: (0, 0, 0)),
            pl.BlockSpec((2, 1, per_device, 2 * ck), lambda k: (0, k, 0, 0)),
        ],
        out_specs=(pl.BlockSpec((block, ck), lambda k: (0, k)),) * 2,
        compiler_params=pltpu.CompilerParams(vmem_limit_bytes=40 * 1024 * 1024),
    )(xg, d_all)
    return grad_t.T, gain_sum[0, :own], grad_gate, grad_up


def solution(mesh):
    in_specs = (
        P("dp", "section"),
        P("dp", ("tp", "section")),
        P(),
        P("dp", ("tp", "section")),
        P("dp", ("tp", "section")),
    )
    out_specs = (
        P("dp", ("tp", "section")),
        P(("tp", "section")),
        P("dp", ("tp", "section")),
        P("dp", ("tp", "section")),
    )
    sizes = tuple(mesh.shape[a] for a in ("dp", "tp", "section"))
    body = fused_shards if sizes == (2, 4, 4) else shards
    return jax.shard_map(body, mesh=mesh, in_specs=in_specs, out_specs=out_specs, check_vma=False)
```
